256 devices in a mesh: seq: 32 (over x, y, core), kvh: 8 (over z).
Axes of the slice: x: 4, y: 4, z: 8, core: 2. Of those that a mesh axis runs over, the one named last changes fastest.
Arguments:
- hidden: bfloat16 [24576, 4096], P('seq'), may hold values from -32 to 32
- w_query: bfloat16 [4096, 4096], P(None, 'kvh'), may hold values from -0.09375 to 0.09375
- w_key: bfloat16 [4096, 1024], P(None, 'kvh'), may hold values from -0.09375 to 0.09375
- w_value: bfloat16 [4096, 1024], P(None, 'kvh'), may hold values from -0.09375 to 0.09375
- cached_key: bfloat16 [24576, 1024], P('seq', 'kvh'), may hold values from -6 to 6
- cached_value: bfloat16 [24576, 1024], P('seq', 'kvh'), may hold values from -6 to 6
- doc_lengths: int32 [4], replicated, may hold values from 1 to 12288, 24576 in all
- selected: int32 [3840], replicated, may hold values from 0 to 767, as said below
Outputs:
- attended: bfloat16 [3840, 4096], P('seq', 'kvh')
- score: float32 [24576], P('seq')
The draws below stay inside these ranges and needn't reach their ends.
Inputs may be any that keep to these rules, and one draw needn't show every extreme that they name: `selected`: each block of 120 entries holds distinct local row numbers in increasing order.
All inputs are finite; a program needn't handle non-finite values.
Results may differ from the reference program's by a relative error of at most 0.02.
Values may be sent and summed in bfloat16 or wider, within the bound.
No kernel may reach another device: no remote copies, remote signals or barrier semaphores. Data moves between devices by JAX's collectives and lax.ppermute only.
A program may use at most 192 MiB of HBM per device.

```python
import math
import jax
import jax.numpy as jnp
import numpy as np
from jax import lax

D = 4096
HEADS = 32
KV_HEADS = 8
HEAD_DIM = 128
TOK_DEV = 768
DOCS = 4
SEL_DEV = 120
TOKENS = 24576
SELECTED = 3840
DOC_MOST = 12288


def draw_selected(key, part):
    blocks = TOKENS // TOK_DEV
    block_keys = jax.random.split(key, blocks)

    def one_block(block_key):
        shuffled = jax.random.permutation(block_key, TOK_DEV)
        return jnp.sort(shuffled[:SEL_DEV]).astype(jnp.int32)
    return jax.vmap(one_block)(block_keys).reshape(-1).astype(jnp.int32)


def draw_hidden(key, part):
    base = jnp.clip(jax.random.normal(key, (TOKENS, D), jnp.float32), -4.0, 4.0)
    region_scale = jnp.exp(jax.random.uniform(jax.random.fold_in(key, 11), (16,), jnp.float32, jnp.log(0.5), jnp.log(2.5)))
    region = jnp.arange(TOKENS, dtype=jnp.int32) * 16 // TOKENS
    base = base * region_scale[region][:, None]
    return base.astype(jnp.bfloat16)


def level_of(stream_key, shape, cuts, low, largest):
    level, own = 1.0, jax.random.fold_in(stream_key, 6)
    for position, parts in cuts:
        heights = jnp.exp(jax.random.uniform(jax.random.fold_in(own, position), (parts,), jnp.float32, low / len(cuts), largest / len(cuts)))
        level = level * jnp.repeat(heights, shape[position] // parts).reshape([-1 if axis == position else 1 for axis in range(len(shape))])
    return level


def profile(number_of, total, bound, skew):
    weights = [(1 << 20) // math.isqrt(standing ** skew) + 1 for standing in range(2, number_of + 1)]
    spare, given = total - bound - (number_of - 1), [1] * (number_of - 1)
    while spare > 0:
        candidates = [i for i in range(number_of - 1) if given[i] < bound]
        pool, budget = sum([weights[i] for i in candidates]), spare
        for i in candidates:
            addition = min(bound - given[i], max(1, budget * weights[i] // pool), spare)
            given[i] = given[i] + addition
            spare = spare - addition
    return np.array([bound] + given)


def ragged_sizes(own_key, amount, total, limit, slope):
    if amount == 2:
        one = jax.random.randint(own_key, (), max(1, total - limit), min(limit, total - 1) + 1)
        return jnp.stack([one, total - one])
    lengths = jnp.asarray(profile(amount, total, limit, slope), jnp.int32)
    pairs = (amount - 1) // 2
    giver, receiver = lengths[1:1 + 2 * pairs:2], lengths[2:2 + 2 * pairs:2]
    margin = jnp.minimum(giver - 1, limit - receiver)
    shifted = jax.random.randint(jax.random.fold_in(own_key, 1), (pairs,), 0, 1 << 20) % (margin + 1)
    lengths = lengths.at[1:1 + 2 * pairs:2].set(giver - shifted).at[2:2 + 2 * pairs:2].set(receiver + shifted)
    return lengths[jax.random.permutation(jax.random.fold_in(own_key, 2), amount)]


def scatter_about(stream_key, extent, width, bound, shards=(), kind=jnp.bfloat16):
    values = jax.random.normal(stream_key, extent, jnp.float32) * width
    if len(shards) > 0:
        values = level_of(stream_key, extent, shards, -0.22, 0.18) * values
    return jnp.clip(values, min=-bound, max=bound).astype(kind)


def setup_inputs(seed: int = 0) -> dict:
    keys = jax.random.split(jax.random.key(seed), 9)
    return {
        "hidden": draw_hidden(jax.random.fold_in(keys[8], 71), 0),
        "w_query": scatter_about(keys[1], (D, HEADS * HEAD_DIM), D ** -0.5, 0.09375, ((1, 8),)),
        "w_key": scatter_about(keys[2], (D, KV_HEADS * HEAD_DIM), D ** -0.5, 0.09375, ((1, 8),)),
        "w_value": scatter_about(keys[3], (D, KV_HEADS * HEAD_DIM), D ** -0.5, 0.09375, ((1, 8),)),
        "cached_key": scatter_about(keys[4], (TOKENS, KV_HEADS * HEAD_DIM), 1.0, 6.0, ((0, 32), (1, 8))),
        "cached_value": scatter_about(keys[5], (TOKENS, KV_HEADS * HEAD_DIM), 1.0, 6.0, ((0, 32), (1, 8))),
        "doc_lengths": ragged_sizes(keys[6], DOCS, TOKENS, DOC_MOST, 2).astype(jnp.int32),
        "selected": draw_selected(jax.random.fold_in(keys[8], 71), 0),
    }


def doc_numbers(positions, doc_lengths):
    boundary = jnp.cumsum(doc_lengths).astype(jnp.int32)
    return jnp.sum((positions[:, None] >= boundary[None, :]).astype(jnp.int32), axis=1).astype(jnp.int32)


def reference(hidden, w_query, w_key, w_value, cached_key, cached_value, doc_lengths, selected):
    group_size = HEADS // KV_HEADS
    scaling = HEAD_DIM ** -0.5
    key_fresh = jnp.dot(hidden, w_key, preferred_element_type=jnp.float32)
    value_fresh = jnp.dot(hidden, w_value, preferred_element_type=jnp.float32)
    key_shift = key_fresh - cached_key.astype(jnp.float32)
    value_shift = value_fresh - cached_value.astype(jnp.float32)
    deviation = jnp.sum(key_shift * key_shift, axis=1) + jnp.sum(value_shift * value_shift, axis=1)
    positions = jnp.arange(TOKENS, dtype=jnp.int32)
    doc_of = doc_numbers(positions, doc_lengths)
    doc_table = (doc_of[:, None] == jnp.arange(DOCS, dtype=jnp.int32)[None, :]).astype(jnp.float32)
    doc_total = jnp.dot(deviation, doc_table, precision=lax.Precision.HIGHEST)
    doc_mean = doc_total / doc_lengths.astype(jnp.float32)
    score = deviation / (jnp.dot(doc_table, doc_mean, precision=lax.Precision.HIGHEST) + 1.0)
    picked = (jnp.arange(SELECTED, dtype=jnp.int32) // SEL_DEV) * TOK_DEV + selected.astype(jnp.int32)
    chosen = jnp.zeros((TOKENS,), jnp.int32).at[picked].set(1) > 0
    key_used = jnp.where(chosen[:, None], key_fresh.astype(jnp.bfloat16), cached_key)
    value_used = jnp.where(chosen[:, None], value_fresh.astype(jnp.bfloat16), cached_value)
    queries = jnp.dot(hidden[picked], w_query, preferred_element_type=jnp.float32).astype(jnp.bfloat16)
    allowed = positions[None, :] <= picked[:, None]
    query_heads = queries.astype(jnp.float32).reshape(SELECTED, HEADS, HEAD_DIM)

    def one_head(head_number):
        query_head = lax.dynamic_index_in_dim(query_heads, head_number, 1, keepdims=False)
        shared = (head_number // group_size).astype(jnp.int32)
        key_head = lax.dynamic_slice_in_dim(key_used, shared * HEAD_DIM, HEAD_DIM, 1).astype(jnp.float32)
        value_head = lax.dynamic_slice_in_dim(value_used, shared * HEAD_DIM, HEAD_DIM, 1).astype(jnp.float32)
        scores = jnp.dot(query_head, key_head.T, precision=lax.Precision.HIGHEST) * scaling
        scores = jnp.where(allowed, scores, -1e30)
        row_max = jnp.max(scores, axis=1, keepdims=True)
        weights = jnp.where(allowed, jnp.exp(scores - row_max), 0.0)
        row_sum = jnp.sum(weights, axis=1, keepdims=True)
        rounded = lax.optimization_barrier(weights.astype(jnp.bfloat16))
        mixed = jnp.dot(rounded.astype(jnp.float32), value_head, precision=lax.Precision.HIGHEST)
        return mixed / row_sum

    heads_out = lax.map(one_head, jnp.arange(HEADS, dtype=jnp.int32))
    attended = jnp.transpose(heads_out, (1, 0, 2)).reshape(SELECTED, HEADS * HEAD_DIM).astype(jnp.bfloat16)
    return attended, score
```

```python
import functools
import math

import jax
import jax.numpy as jnp
from jax import lax
from jax.experimental import pallas as pl
from jax.experimental.pallas import tpu as pltpu
from jax.sharding import Mesh, PartitionSpec as P

HEADS = 32
KV_HEADS = 8
HEAD_DIM = 128
GROUP = 4
TOK = 768
SEL = 120
ROWS = 128
QROWS = GROUP * ROWS
DOCS = 4
CHUNK = 512
NEG = -1e30
EXP_SCALE = (HEAD_DIM ** -0.5) * math.log2(math.e)
SEQ = ("x", "y", "c")
f32, bf16 = jnp.float32, jnp.bfloat16


def seq_number():
    return (lax.axis_index("x") * 4 + lax.axis_index("y")) * 2 + lax.axis_index("c")


def doc_ends(lengths):
    ends = [lengths[0]]
    for d in range(1, DOCS):
        ends.append(ends[-1] + lengths[d])
    return ends


def project_kernel(lengths, own, hidden, w_query, w_key, w_value, cached_key, cached_value,
                   kv_out, q_out, dev_out, pick, acc_kv, acc_q):
    step = pl.program_id(0)

    @pl.when(step == 0)
    def _():
        across = jnp.broadcast_to(own[...], (ROWS, ROWS)).astype(f32).T
        tokens = lax.broadcasted_iota(jnp.int32, (ROWS, TOK), 1).astype(f32)
        wide = jnp.concatenate([across] * (TOK // ROWS), axis=1)
        pick[...] = jnp.where(wide == tokens, 1.0, 0.0).astype(bf16)
        acc_kv[...] = jnp.zeros_like(acc_kv)
        acc_q[...] = jnp.zeros_like(acc_q)

    states = hidden[...]
    both = jnp.concatenate([w_key[...], w_value[...]], axis=1)
    acc_kv[...] += jnp.dot(states, both, preferred_element_type=f32)
    picked = jnp.dot(pick[...], states, preferred_element_type=f32).astype(bf16)
    acc_q[...] += jnp.dot(picked, w_query[...], preferred_element_type=f32)

    @pl.when(step == pl.num_programs(0) - 1)
    def _():
        tokens = lax.broadcasted_iota(jnp.int32, (TOK, ROWS), 0)
        hit = jnp.where(tokens == own[...], 1.0, 0.0)
        chosen = jnp.max(hit, axis=1, keepdims=True) > 0.0
        old_key = cached_key[...].astype(f32)
        old_value = cached_value[...].astype(f32)
        new_key = acc_kv[:, :HEAD_DIM]
        new_value = acc_kv[:, HEAD_DIM:]
        kv_out[:TOK, :] = jnp.where(chosen, new_key, old_key).astype(bf16)
        value_used = jnp.where(chosen, new_value, old_value)
        for t in range(TOK // ROWS):
            kv_out[TOK + t * ROWS:TOK + (t + 1) * ROWS, :] = (
                value_used[t * ROWS:(t + 1) * ROWS, :].T.astype(bf16))
        for h in range(GROUP):
            q_out[h * ROWS:(h + 1) * ROWS, :] = acc_q[:, h * HEAD_DIM:(h + 1) * HEAD_DIM].astype(bf16)
        shift = (new_key - old_key) ** 2 + (new_value - old_value) ** 2
        first = seq_number() * TOK
        ends = doc_ends(lengths)
        lane = lax.broadcasted_iota(jnp.int32, (1, ROWS), 1)
        totals = [jnp.zeros((1, ROWS), f32) for _ in range(DOCS)]
        for t in range(TOK // ROWS):
            dev = jnp.sum(shift[t * ROWS:(t + 1) * ROWS, :].T, axis=0, keepdims=True)
            dev_out[t:t + 1, :] = dev
            place = lane + (first + t * ROWS)
            doc = sum([(place >= e).astype(jnp.int32) for e in ends])
            for d in range(DOCS):
                totals[d] = totals[d] + jnp.where(doc == d, dev, 0.0)
        row = jnp.zeros((1, ROWS), f32)
        for d in range(DOCS):
            row = jnp.where(lane == d, jnp.sum(totals[d], axis=1, keepdims=True), row)
        dev_out[6:7, :] = row
        dev_out[7:8, :] = jnp.zeros((1, ROWS), f32)


def project(lengths, own, hidden, w_query, w_key, w_value, cached_key, cached_value):
    steps = hidden.shape[1] // CHUNK
    whole = lambda k: (0, 0)
    return pl.pallas_call(
        project_kernel,
        grid=(steps,),
        in_specs=[
            pl.BlockSpec(memory_space=pltpu.SMEM),
            pl.BlockSpec((1, ROWS), whole),
            pl.BlockSpec((TOK, CHUNK), lambda k: (0, k)),
            pl.BlockSpec((CHUNK, GROUP * HEAD_DIM), lambda k: (k, 0)),
            pl.BlockSpec((CHUNK, HEAD_DIM), lambda k: (k, 0)),
            pl.BlockSpec((CHUNK, HEAD_DIM), lambda k: (k, 0)),
            pl.BlockSpec((TOK, HEAD_DIM), whole),
            pl.BlockSpec((TOK, HEAD_DIM), whole),
        ],
        out_specs=[
            pl.BlockSpec((2 * TOK, HEAD_DIM), whole),
            pl.BlockSpec((QROWS, HEAD_DIM), whole),
            pl.BlockSpec((8, ROWS), whole),
        ],
        out_shape=[
            jax.ShapeDtypeStruct((2 * TOK, HEAD_DIM), bf16),
            jax.ShapeDtypeStruct((QROWS, HEAD_DIM), bf16),
            jax.ShapeDtypeStruct((8, ROWS), f32),
        ],
        scratch_shapes=[
            pltpu.VMEM((ROWS, TOK), bf16),
            pltpu.VMEM((TOK, 2 * HEAD_DIM), f32),
            pltpu.VMEM((ROWS, GROUP * HEAD_DIM), f32),
        ],
        compiler_params=pltpu.CompilerParams(vmem_limit_bytes=24 * 2**20),
        cost_estimate=pl.CostEstimate(flops=2 * 10**9, bytes_accessed=13 * 10**6, transcendentals=0),
        name="project",
    )(lengths, own, hidden, w_query, w_key, w_value, cached_key, cached_value)


X_STEPS = (0, 1, 3, 2)
Y_STEPS = (0, 1, 3, 2)
QT = 256


def attend_pair(q, kv, m_s, l_s, acc_s, i, j, mask_rows):
    keys = kv[j, :TOK, :]
    for t in range(QROWS // QT):
        cols = slice(t * QT, (t + 1) * QT)
        s = lax.dot_general(keys, q[i, cols, :], (((1,), (1,)), ((), ())), preferred_element_type=f32)
        if mask_rows is not None:
            place = lax.broadcasted_iota(jnp.int32, (TOK, QT), 0)
            s = jnp.where(place <= mask_rows[:, cols], s, NEG)
        old = m_s[i, 0:1, cols]
        new = jnp.maximum(old, jnp.max(s, axis=0, keepdims=True))
        p = jnp.exp2((s - new) * EXP_SCALE)
        fade = jnp.exp2((old - new) * EXP_SCALE)
        m_s[i, 0:1, cols] = new
        l_s[i, 0:1, cols] = l_s[i, 0:1, cols] * fade + jnp.sum(p, axis=0, keepdims=True)
        pb = p.astype(bf16)
        mixed = acc_s[i, :, cols] * fade
        values = jnp.concatenate(
            [kv[j, TOK + k * ROWS:TOK + (k + 1) * ROWS, :] for k in range(TOK // ROWS)], axis=1)
        acc_s[i, :, cols] = mixed + jnp.dot(values, pb, preferred_element_type=f32)


def attend_kernel(mask_rows, *refs):
    q_in, kv_in, outs = refs[:4], refs[4:12], refs[12:16]
    q, kv, m_s, l_s, acc_s, q_sem, kv_sem = refs[16:]
    q_copies = [pltpu.make_async_copy(q_in[i], q.at[i], q_sem.at[i]) for i in range(4)]
    kv_copies = [pltpu.make_async_copy(kv_in[j], kv.at[j], kv_sem.at[j]) for j in range(8)]
    q_copies[0].start()
    kv_copies[0].start()
    for c in q_copies[1:] + kv_copies[1:]:
        c.start()
    m_s[...] = jnp.full_like(m_s, NEG)
    l_s[...] = jnp.zeros_like(l_s)
    acc_s[...] = jnp.zeros_like(acc_s)
    x, y, c = lax.axis_index("x"), lax.axis_index("y"), lax.axis_index("c")
    for copy in q_copies:
        copy.wait()
    kv_copies[0].wait()
    attend_pair(q, kv, m_s, l_s, acc_s, 0, 0, mask_rows)
    for copy in kv_copies[1:]:
        copy.wait()

    @pl.loop(0, 32)
    def _(n):
        i = n // 8
        j = n % 8
        dx = jnp.where(i == 2, 3, jnp.where(i == 3, 2, i))
        k = j // 2
        dy = jnp.where(k == 2, 3, jnp.where(k == 3, 2, k))
        q_at = ((x + dx) % 4) * 8 + 2 * y + c
        kv_at = x * 8 + 2 * ((y + dy) % 4) + (c + j % 2) % 2

        @pl.when(q_at > kv_at)
        def _():
            attend_pair(q, kv, m_s, l_s, acc_s, i, j, None)

    for i in range(4):
        total = l_s[i, 0:1, :]
        outs[i][:HEAD_DIM, :] = (acc_s[i] / jnp.maximum(total, 1e-30)).astype(bf16)
        lse = jnp.where(total > 0.0, m_s[i, 0:1, :] * EXP_SCALE + jnp.log2(jnp.maximum(total, 1e-30)), NEG)
        high = lse.astype(bf16)
        rest = lse - high.astype(f32)
        mid = rest.astype(bf16)
        low = (rest - mid.astype(f32)).astype(bf16)
        outs[i][HEAD_DIM:, :] = jnp.concatenate(
            [high.astype(f32), mid.astype(f32), low.astype(f32), jnp.zeros((13, QROWS), f32)], axis=0).astype(bf16)


def attend(mask_rows, qs, kvs):
    hbm = pl.BlockSpec(memory_space=pltpu.HBM)
    vmem = pl.BlockSpec(memory_space=pltpu.VMEM)
    return pl.pallas_call(
        attend_kernel,
        in_specs=[vmem] + [hbm] * 12,
        out_specs=[vmem] * 4,
        out_shape=[jax.ShapeDtypeStruct((HEAD_DIM + 16, QROWS), bf16)] * 4,
        scratch_shapes=[
            pltpu.VMEM((4, QROWS, HEAD_DIM), bf16),
            pltpu.VMEM((8, 2 * TOK, HEAD_DIM), bf16),
            pltpu.VMEM((4, 8, QROWS), f32),
            pltpu.VMEM((4, 8, QROWS), f32),
            pltpu.VMEM((4, HEAD_DIM, QROWS), f32),
            pltpu.SemaphoreType.DMA((4,)),
            pltpu.SemaphoreType.DMA((8,)),
        ],
        compiler_params=pltpu.CompilerParams(vmem_limit_bytes=40 * 2**20),
        cost_estimate=pl.CostEstimate(flops=12 * 10**9, bytes_accessed=4 * 10**6, transcendentals=12 * 10**6),
        name="attend",
    )(mask_rows, *qs, *kvs)


def combine_kernel(lengths, dev, p0, p1, p2, p3, out, score):
    parts = (p0, p1, p2, p3)
    lses = [p[HEAD_DIM:HEAD_DIM + 16, :].astype(f32) for p in parts]
    lses = [v[0:1] + v[1:2] + v[2:3] for v in lses]
    top = functools.reduce(jnp.maximum, lses)
    weights = [jnp.exp2(v - top) for v in lses]
    scale = 1.0 / sum(weights)
    mixed = sum([p[:HEAD_DIM, :].astype(f32) * (w * scale) for p, w in zip(parts, weights)])
    for h in range(GROUP):
        out[:, h * HEAD_DIM:(h + 1) * HEAD_DIM] = (
            mixed[:, h * ROWS:(h + 1) * ROWS].T[:SEL, :].astype(bf16))
    first = seq_number() * TOK
    ends = doc_ends(lengths)
    lane = lax.broadcasted_iota(jnp.int32, (8, ROWS), 1)
    place = lane + lax.broadcasted_iota(jnp.int32, (8, ROWS), 0) * ROWS + first
    doc = sum([(place >= e).astype(jnp.int32) for e in ends])
    mean = jnp.zeros((8, ROWS), f32)
    for d in range(DOCS):
        mean = jnp.where(doc == d, dev[6:7, d:d + 1] / lengths[d].astype(f32), mean)
    score[...] = dev[...] / (mean + 1.0)


def combine(lengths, dev, parts):
    vmem = pl.BlockSpec(memory_space=pltpu.VMEM)
    return pl.pallas_call(
        combine_kernel,
        in_specs=[pl.BlockSpec(memory_space=pltpu.SMEM)] + [vmem] * 5,
        out_specs=[vmem, vmem],
        out_shape=[
            jax.ShapeDtypeStruct((SEL, GROUP * HEAD_DIM), bf16),
            jax.ShapeDtypeStruct((8, ROWS), f32),
        ],
        compiler_params=pltpu.CompilerParams(vmem_limit_bytes=8 * 2**20),
        cost_estimate=pl.CostEstimate(flops=10**6, bytes_accessed=10**6, transcendentals=0),
        name="combine",
    )(lengths, dev, *parts)


def fetch(value, axis, step):
    size = lax.axis_size(axis)
    return lax.ppermute(value, axis, [((i + step) % size, i) for i in range(size)])


def exchange(value, axis, bit):
    size = lax.axis_size(axis)
    return lax.ppermute(value, axis, [(i, i ^ bit) for i in range(size)])


def shards(hidden, w_query, w_key, w_value, cached_key, cached_value, doc_lengths, selected):
    own = lax.dynamic_slice_in_dim(selected, seq_number() * SEL, SEL, 0)
    rows = jnp.pad(own, (0, ROWS - SEL), constant_values=-1)[None, :]
    mask_rows = jnp.tile(jnp.pad(own, (0, ROWS - SEL), constant_values=TOK)[None, :], (1, GROUP))
    kv, q, dev = project(doc_lengths, rows, hidden, w_query, w_key, w_value, cached_key, cached_value)
    kv_y = [kv] + [fetch(kv, "y", s) for s in Y_STEPS[1:]]
    qs = [q] + [fetch(q, "x", s) for s in X_STEPS[1:]]
    kvs = []
    for block in kv_y:
        kvs += [block, exchange(block, "c", 1)]
    for bit in (1, 2, 4):
        dev = dev + exchange(dev, "kvh", bit)
    docs = dev
    for axis, bit in (("c", 1), ("y", 1), ("y", 2), ("x", 1), ("x", 2)):
        docs = docs + exchange(docs, axis, bit)
    dev = jnp.concatenate([dev[:6], docs[6:]], axis=0)
    parts = attend(mask_rows, qs, kvs)
    mine = [parts[0]]
    for n, s in enumerate(X_STEPS[1:]):
        back = (4 - s) % 4
        mine.append(fetch(parts[n + 1], "x", back))
    attended, score = combine(doc_lengths, dev, mine)
    return attended, score.reshape(-1)[:TOK]


def solution(mesh):
    fine = Mesh(mesh.devices.reshape(4, 4, 2, 8), ("x", "y", "c", "kvh"))
    return jax.shard_map(
        shards,
        mesh=fine,
        in_specs=(
            P(SEQ, None),
            P(None, "kvh"),
            P(None, "kvh"),
            P(None, "kvh"),
            P(SEQ, "kvh"),
            P(SEQ, "kvh"),
            P(),
            P(),
        ),
        out_specs=(P(SEQ, "kvh"), P(SEQ)),
        check_vma=False,
    )
```

```python
import functools
import math

import jax
import jax.numpy as jnp
from jax import lax
from jax.experimental import pallas as pl
from jax.experimental.pallas import tpu as pltpu
from jax.sharding import Mesh, PartitionSpec as P


HEAD_DIM = 128
GROUP = 4
TOK = 768
SEL = 120
ROWS = 128
QROWS = GROUP * ROWS
DOCS = 4
CHUNK = 1024
NEG = -1e30
EXP_SCALE = (HEAD_DIM ** -0.5) * math.log2(math.e)
SEQ = ("x", "y", "c")
f32, bf16 = jnp.float32, jnp.bfloat16


def seq_number():
    return (lax.axis_index("x") * 4 + lax.axis_index("y")) * 2 + lax.axis_index("c")


def doc_ends(lengths):
    ends = [lengths[0]]
    for d in range(1, DOCS):
        ends.append(ends[-1] + lengths[d])
    return ends


def project_kernel(lengths, selected, hidden, w_query, w_key, w_value, cached_key, cached_value,
                   kv_out, q_out, dev_out, mask_out,
                   states, wq, wkv, old, chosen_rows, acc_kv, acc_q, sem, one_sem):
    steps = hidden.shape[1] // CHUNK
    fetch_rows = pltpu.make_async_copy(selected, chosen_rows, one_sem.at[0])
    fetch_rows.start()
    copies = []
    for k in range(steps):
        part = pl.ds(k * CHUNK, CHUNK)
        copies.append([
            pltpu.make_async_copy(hidden.at[:, part], states.at[k], sem.at[0, k]),
            pltpu.make_async_copy(w_key.at[part, :], wkv.at[k, :, pl.ds(0, HEAD_DIM)], sem.at[1, k]),
            pltpu.make_async_copy(w_value.at[part, :], wkv.at[k, :, pl.ds(HEAD_DIM, HEAD_DIM)], sem.at[2, k]),
            pltpu.make_async_copy(w_query.at[part, :], wq.at[k], sem.at[3, k]),
        ])
        for copy in copies[-1]:
            copy.start()
    olds = [
        pltpu.make_async_copy(cached_key, old.at[0], one_sem.at[1]),
        pltpu.make_async_copy(cached_value, old.at[1], one_sem.at[2]),
    ]
    for copy in olds:
        copy.start()
    fetch_rows.wait()
    base = seq_number() * SEL
    lane = lax.broadcasted_iota(jnp.int32, (1, ROWS), 1)
    pieces = [jnp.full((1, ROWS), -1, jnp.int32) for _ in range(4)]
    for r in range(SEL):
        pieces[r % 4] = jnp.where(lane == r, chosen_rows[base + r], pieces[r % 4])
    own = functools.reduce(jnp.maximum, pieces)
    mask_out[...] = jnp.concatenate([jnp.where(lane < SEL, own, TOK)] * GROUP, axis=1)
    across = jnp.broadcast_to(own, (ROWS, ROWS)).astype(f32).T
    tokens = lax.broadcasted_iota(jnp.int32, (ROWS, TOK), 1).astype(f32)
    pick = jnp.where(jnp.concatenate([across] * (TOK // ROWS), axis=1) == tokens, 1.0, 0.0).astype(bf16)
    acc_kv[...] = jnp.zeros_like(acc_kv)
    acc_q[...] = jnp.zeros_like(acc_q)
    for k in range(steps):
        for copy in copies[k]:
            copy.wait()
        acc_kv[...] += jnp.dot(states[k], wkv[k], preferred_element_type=f32)
        picked = jnp.dot(pick, states[k], preferred_element_type=f32).astype(bf16)
        acc_q[...] += jnp.dot(picked, wq[k], preferred_element_type=f32)
    for copy in olds:
        copy.wait()
    for h in range(GROUP):
        q_out[h * ROWS:(h + 1) * ROWS, :] = (
            acc_q[:, h * HEAD_DIM:(h + 1) * HEAD_DIM] * EXP_SCALE).astype(bf16)
    first = seq_number() * TOK
    ends = doc_ends(lengths)
    totals = [jnp.zeros((1, ROWS), f32) for _ in range(DOCS)]
    for t in range(TOK // ROWS):
        part = slice(t * ROWS, (t + 1) * ROWS)
        place = lax.broadcasted_iota(jnp.int32, (ROWS, ROWS), 0) + t * ROWS
        chosen = jnp.max(jnp.where(place == own, 1.0, 0.0), axis=1, keepdims=True) > 0.0
        old_key = old[0, part, :].astype(f32)
        old_value = old[1, part, :].astype(f32)
        new_key = acc_kv[part, :HEAD_DIM]
        new_value = acc_kv[part, HEAD_DIM:]
        kv_out[part, :] = jnp.where(chosen, new_key, old_key).astype(bf16)
        kv_out[TOK + t * ROWS:TOK + (t + 1) * ROWS, :] = jnp.where(chosen, new_value, old_value).T.astype(bf16)
        shift = (new_key - old_key) ** 2 + (new_value - old_value) ** 2
        dev = jnp.sum(shift.T, axis=0, keepdims=True)
        dev_out[t:t + 1, :] = dev
        at = lane + (first + t * ROWS)
        doc = sum([(at >= e).astype(jnp.int32) for e in ends])
        for d in range(DOCS):
            totals[d] = totals[d] + jnp.where(doc == d, dev, 0.0)
    row = jnp.zeros((1, ROWS), f32)
    for d in range(DOCS):
        row = jnp.where(lane == d, jnp.sum(totals[d], axis=1, keepdims=True), row)
    dev_out[6:7, :] = row
    dev_out[7:8, :] = jnp.zeros((1, ROWS), f32)


def project(lengths, selected, hidden, w_query, w_key, w_value, cached_key, cached_value):
    steps = hidden.shape[1] // CHUNK
    hbm = pl.BlockSpec(memory_space=pltpu.HBM)
    vmem = pl.BlockSpec(memory_space=pltpu.VMEM)
    return pl.pallas_call(
        project_kernel,
        in_specs=[pl.BlockSpec(memory_space=pltpu.SMEM)] + [hbm] * 7,
        out_specs=[vmem] * 4,
        out_shape=[
            jax.ShapeDtypeStruct((2 * TOK, HEAD_DIM), bf16),
            jax.ShapeDtypeStruct((QROWS, HEAD_DIM), bf16),
            jax.ShapeDtypeStruct((8, ROWS), f32),
            jax.ShapeDtypeStruct((1, QROWS), jnp.int32),
        ],
        scratch_shapes=[
            pltpu.VMEM((steps, TOK, CHUNK), bf16),
            pltpu.VMEM((steps, CHUNK, GROUP * HEAD_DIM), bf16),
            pltpu.VMEM((steps, CHUNK, 2 * HEAD_DIM), bf16),
            pltpu.VMEM((2, TOK, HEAD_DIM), bf16),
            pltpu.SMEM(selected.shape, jnp.int32),
            pltpu.VMEM((TOK, 2 * HEAD_DIM), f32),
            pltpu.VMEM((ROWS, GROUP * HEAD_DIM), f32),
            pltpu.SemaphoreType.DMA((4, steps)),
            pltpu.SemaphoreType.DMA((3,)),
        ],
        compiler_params=pltpu.CompilerParams(vmem_limit_bytes=66_400_000),
        cost_estimate=pl.CostEstimate(flops=5 * 10**9, bytes_accessed=13 * 10**6, transcendentals=0),
        name="project",
    )(lengths, selected, hidden, w_query, w_key, w_value, cached_key, cached_value)


X_STEPS = (0, 1, 3, 2)
Y_STEPS = (0, 1, 3, 2)
ACC = HEAD_DIM + 16


def score_tile(q, kv, i, j, s_ref, top_ref):
    s = lax.dot_general(kv[j, :TOK, :], q[i], (((1,), (1,)), ((), ())), preferred_element_type=f32)
    s_ref[...] = s
    top_ref[...] = jnp.max(s.reshape(TOK // 8, 8, QROWS), axis=0)


def mix_tile(kv, m_s, acc_s, i, j, s_ref, top_ref):
    old = m_s[i, 0:1, :]
    new = jnp.maximum(old, jnp.max(top_ref[...], axis=0, keepdims=True))
    m_s[i, 0:1, :] = new
    p = jnp.exp2(s_ref[...] - new).astype(bf16)
    values = jnp.concatenate(
        [kv[j, TOK + k * ROWS:TOK + (k + 1) * ROWS, :] for k in range(TOK // ROWS)], axis=1)
    values = jnp.concatenate([values, jnp.ones((16, TOK), bf16)], axis=0)
    acc_s[i] = acc_s[i] * jnp.exp2(old - new) + jnp.dot(values, p, preferred_element_type=f32)


def attend_kernel(dy, first, last, *refs):
    n = 2
    refs = list(refs)
    mask_rows = refs.pop(0) if first else None
    q_in, refs = refs[:4], refs[4:]
    kv_in, refs = refs[:n], refs[n:]
    if not first:
        m_in, acc_in, refs = refs[0], refs[1], refs[2:]
    if last:
        outs, refs = refs[:4], refs[4:]
        m_s, acc_s, refs = refs[0], refs[1], refs[2:]
    else:
        m_s, acc_s, refs = refs[0], refs[1], refs[2:]
    q, kv, s_a, s_b, top_a, top_b, pairs = refs
    for i in range(4):
        q[i] = q_in[i][...]
    for j in range(n):
        kv[j] = kv_in[j][...]
    if first:
        m_s[...] = jnp.full_like(m_s, NEG)
        acc_s[...] = jnp.zeros_like(acc_s)
        place = lax.broadcasted_iota(jnp.int32, (TOK, QROWS), 0)
        s = lax.dot_general(kv[0, :TOK, :], q[0], (((1,), (1,)), ((), ())), preferred_element_type=f32)
        s = jnp.where(place <= mask_rows[...], s, NEG)
        s_a[...] = s
        top_a[...] = jnp.max(s.reshape(TOK // 8, 8, QROWS), axis=0)
        mix_tile(kv, m_s, acc_s, 0, 0, s_a, top_a)
    else:
        m_s[...] = m_in[...]
        acc_s[...] = acc_in[...]
    x, y, c = lax.axis_index("x"), lax.axis_index("y"), lax.axis_index("c")
    count = jnp.int32(0)
    for i, dx in enumerate(X_STEPS):
        for j, dc in enumerate((0, 1)):
            q_at = ((x + dx) & 3) * 8 + 2 * y + c
            kv_at = x * 8 + 2 * ((y + dy) & 3) + ((c + dc) & 1)
            pairs[count] = i * 8 + j
            count = count + jnp.where(q_at > kv_at, 1, 0)

    def pair(k):
        v = pairs[jnp.minimum(k, count - 1)]
        return v >> 3, v & 7

    @pl.when(count > 0)
    def _():
        score_tile(q, kv, *pair(0), s_a, top_a)

    @pl.loop(0, (count + 1) >> 1)
    def _(h):
        k = h * 2
        score_tile(q, kv, *pair(k + 1), s_b, top_b)
        mix_tile(kv, m_s, acc_s, *pair(k), s_a, top_a)

        @pl.when(k + 1 < count)
        def _():
            score_tile(q, kv, *pair(k + 2), s_a, top_a)
            mix_tile(kv, m_s, acc_s, *pair(k + 1), s_b, top_b)

    if last:
        for i in range(4):
            total = acc_s[i, HEAD_DIM:HEAD_DIM + 1, :]
            safe = jnp.maximum(total, 1e-30)
            outs[i][:HEAD_DIM, :] = (acc_s[i, :HEAD_DIM, :] * (1.0 / safe)).astype(bf16)
            lse = jnp.where(total > 0.0, m_s[i, 0:1, :] + jnp.log2(safe), NEG)
            outs[i][HEAD_DIM:, :] = jnp.concatenate(
                split3(lse) + [jnp.zeros((13, QROWS), f32)], axis=0).astype(bf16)


def split3(value):
    high = value.astype(bf16).astype(f32)
    mid = (value - high).astype(bf16).astype(f32)
    return [high, mid, value - high - mid]


def attend(dy, last, qs, kvs, mask_rows, state):
    first = state is None
    n = 2
    vmem = pl.BlockSpec(memory_space=pltpu.VMEM)
    args = ([mask_rows] if first else []) + list(qs) + list(kvs)
    args += [] if first else list(state)
    states = [jax.ShapeDtypeStruct((4, 8, QROWS), f32), jax.ShapeDtypeStruct((4, ACC, QROWS), f32)]
    keep = [pltpu.VMEM((4, 8, QROWS), f32), pltpu.VMEM((4, ACC, QROWS), f32)]
    return pl.pallas_call(
        functools.partial(attend_kernel, dy, first, last),
        in_specs=[vmem] * len(args),
        out_specs=[vmem] * (4 if last else 2),
        out_shape=[jax.ShapeDtypeStruct((ACC, QROWS), bf16)] * 4 if last else states,
        scratch_shapes=(keep if last else []) + [
            pltpu.VMEM((4, QROWS, HEAD_DIM), bf16),
            pltpu.VMEM((n, 2 * TOK, HEAD_DIM), bf16),
            pltpu.VMEM((TOK, QROWS), f32),
            pltpu.VMEM((TOK, QROWS), f32),
            pltpu.VMEM((8, QROWS), f32),
            pltpu.VMEM((8, QROWS), f32),
            pltpu.SMEM((40,), jnp.int32),
        ],
        compiler_params=pltpu.CompilerParams(vmem_limit_bytes=30 * 2**20),
        cost_estimate=pl.CostEstimate(flops=n * 4 * 10**9, bytes_accessed=4 * 10**6, transcendentals=10**6),
        name="attend",
    )(*args)


def combine_kernel(lengths, dev, docs, p0, p1, p2, p3, out, score):
    parts = (p0, p1, p2, p3)
    rows = [p[HEAD_DIM:HEAD_DIM + 16, :].astype(f32) for p in parts]
    lses = [v[0:1] + v[1:2] + v[2:3] for v in rows]
    total = docs[6:7, :]
    top = functools.reduce(jnp.maximum, lses)
    weights = [jnp.exp2(v - top) for v in lses]
    scale = 1.0 / sum(weights)
    mixed = sum([p[:HEAD_DIM, :].astype(f32) * (w * scale) for p, w in zip(parts, weights)])
    for h in range(GROUP):
        out[:, h * HEAD_DIM:(h + 1) * HEAD_DIM] = (
            mixed[:, h * ROWS:(h + 1) * ROWS].T[:SEL, :].astype(bf16))
    first = seq_number() * TOK
    ends = doc_ends(lengths)
    lane = lax.broadcasted_iota(jnp.int32, (8, ROWS), 1)
    place = lane + lax.broadcasted_iota(jnp.int32, (8, ROWS), 0) * ROWS + first
    doc = sum([(place >= e).astype(jnp.int32) for e in ends])
    mean = jnp.zeros((8, ROWS), f32)
    for d in range(DOCS):
        mean = jnp.where(doc == d, total[:, d:d + 1] / lengths[d].astype(f32), mean)
    score[...] = dev[...] / (mean + 1.0)


def combine(lengths, dev, docs, parts):
    vmem = pl.BlockSpec(memory_space=pltpu.VMEM)
    return pl.pallas_call(
        combine_kernel,
        in_specs=[pl.BlockSpec(memory_space=pltpu.SMEM)] + [vmem] * 6,
        out_specs=[vmem, vmem],
        out_shape=[
            jax.ShapeDtypeStruct((SEL, GROUP * HEAD_DIM), bf16),
            jax.ShapeDtypeStruct((8, ROWS), f32),
        ],
        compiler_params=pltpu.CompilerParams(vmem_limit_bytes=8 * 2**20),
        cost_estimate=pl.CostEstimate(flops=10**6, bytes_accessed=10**6, transcendentals=0),
        name="combine",
    )(lengths, dev, docs, *parts)


def fetch(value, axis, step):
    size = lax.axis_size(axis)
    return lax.ppermute(value, axis, [((i + step) % size, i) for i in range(size)])


def exchange(value, axis, bit):
    size = lax.axis_size(axis)
    return lax.ppermute(value, axis, [(i, i ^ bit) for i in range(size)])


def program(hidden, w_query, w_key, w_value, cached_key, cached_value, doc_lengths, selected):
    kv, q, dev, mask_rows = project(
        doc_lengths, selected, hidden, w_query, w_key, w_value, cached_key, cached_value)
    kv_y, kv_c, qs = {0: kv}, {}, [q]
    for s in (1, 3, 2):
        kv_y[s] = fetch(kv, "y", s)
    for s in X_STEPS[1:]:
        qs.append(fetch(q, "x", s))
    for s in (0, 1, 3, 2):
        kv_c[s] = exchange(kv_y[s], "c", 1)
    for bit in (1, 2, 4):
        dev = dev + exchange(dev, "kvh", bit)
    docs = dev
    for axis, bit in (("c", 1), ("y", 1), ("y", 2), ("x", 1), ("x", 2)):
        docs = docs + exchange(docs, axis, bit)
    state = None
    for n, s in enumerate(Y_STEPS):
        state = attend(s, n == len(Y_STEPS) - 1, qs, [kv_y[s], kv_c[s]], mask_rows, state)
    mine = [state[0]]
    for n, s in enumerate(X_STEPS[1:]):
        mine.append(fetch(state[n + 1], "x", (4 - s) % 4))
    attended, score = combine(doc_lengths, dev, docs, mine)
    return attended, score.reshape(-1)[:TOK]


def solution(mesh):
    fine = Mesh(mesh.devices.reshape(4, 4, 2, 8), ("x", "y", "c", "kvh"))
    return jax.shard_map(
        program,
        mesh=fine,
        in_specs=(
            P(SEQ, None),
            P(None, "kvh"),
            P(None, "kvh"),
            P(None, "kvh"),
            P(SEQ, "kvh"),
            P(SEQ, "kvh"),
            P(),
            P(),
        ),
        out_specs=(P(SEQ, "kvh"), P(SEQ)),
        check_vma=False,
    )
```

```python
import functools
import math

import jax
import jax.numpy as jnp
from jax import lax
from jax.experimental import pallas as pl
from jax.experimental.pallas import tpu as pltpu
from jax.sharding import Mesh, PartitionSpec as P


HEAD_DIM = 128
GROUP = 4
TOK = 768
SEL = 120
ROWS = 128
QROWS = GROUP * ROWS
DOCS = 4
CHUNK = 1024
NEG = -1e30
VMEM_PROJECT = 66_000_000
KV_ROWS = 2 * TOK
EXP_SCALE = (HEAD_DIM ** -0.5) * math.log2(math.e)
SEQ = ("x", "y", "c")
f32, bf16 = jnp.float32, jnp.bfloat16


def seq_number():
    return (lax.axis_index("x") * 4 + lax.axis_index("y")) * 2 + lax.axis_index("c")


def doc_ends(lengths):
    ends = [lengths[0]]
    for d in range(1, DOCS):
        ends.append(ends[-1] + lengths[d])
    return ends


def project_kernel(lengths, selected, hidden, w_query, w_key, w_value, cached_key, cached_value,
                   kv_out, q_out, dev_out, mask_out,
                   states, wq, wkv, old, chosen_rows, acc_kv, acc_q, sem, one_sem):
    steps = hidden.shape[1] // CHUNK
    fetch_rows = pltpu.make_async_copy(selected, chosen_rows, one_sem.at[0])
    fetch_rows.start()
    copies = []
    for k in range(steps):
        part = pl.ds(k * CHUNK, CHUNK)
        copies.append([
            pltpu.make_async_copy(hidden.at[:, part], states.at[k], sem.at[0, k]),
            pltpu.make_async_copy(w_key.at[part, :], wkv.at[k, :, pl.ds(0, HEAD_DIM)], sem.at[1, k]),
            pltpu.make_async_copy(w_value.at[part, :], wkv.at[k, :, pl.ds(HEAD_DIM, HEAD_DIM)], sem.at[2, k]),
            pltpu.make_async_copy(w_query.at[part, :], wq.at[k], sem.at[3, k]),
        ])
        for copy in copies[-1]:
            copy.start()
    olds = [
        pltpu.make_async_copy(cached_key, old.at[0], one_sem.at[1]),
        pltpu.make_async_copy(cached_value, old.at[1], one_sem.at[2]),
    ]
    for copy in olds:
        copy.start()
    fetch_rows.wait()
    base = seq_number() * SEL
    lane = lax.broadcasted_iota(jnp.int32, (1, ROWS), 1)
    pieces = [jnp.full((1, ROWS), -1, jnp.int32) for _ in range(4)]
    for r in range(SEL):
        pieces[r % 4] = jnp.where(lane == r, chosen_rows[base + r], pieces[r % 4])
    own = functools.reduce(jnp.maximum, pieces)
    mask_out[...] = jnp.concatenate([jnp.where(lane < SEL, own, TOK)] * GROUP, axis=1)
    across = jnp.broadcast_to(own, (ROWS, ROWS)).astype(f32).T
    tokens = lax.broadcasted_iota(jnp.int32, (ROWS, TOK), 1).astype(f32)
    pick = jnp.where(jnp.concatenate([across] * (TOK // ROWS), axis=1) == tokens, 1.0, 0.0).astype(bf16)
    acc_kv[...] = jnp.zeros_like(acc_kv)
    acc_q[...] = jnp.zeros_like(acc_q)
    for k in range(steps):
        for copy in copies[k]:
            copy.wait()
        acc_kv[...] += jnp.dot(states[k], wkv[k], preferred_element_type=f32)
        picked = jnp.dot(pick, states[k], preferred_element_type=f32).astype(bf16)
        acc_q[...] += jnp.dot(picked, wq[k], preferred_element_type=f32)
    for copy in olds:
        copy.wait()
    for h in range(GROUP):
        q_out[h * ROWS:(h + 1) * ROWS, :] = (
            acc_q[:, h * HEAD_DIM:(h + 1) * HEAD_DIM] * EXP_SCALE).astype(bf16)
    first = seq_number() * TOK
    ends = doc_ends(lengths)
    totals = [jnp.zeros((1, ROWS), f32) for _ in range(DOCS)]
    for t in range(TOK // ROWS):
        part = slice(t * ROWS, (t + 1) * ROWS)
        place = lax.broadcasted_iota(jnp.int32, (ROWS, ROWS), 0) + t * ROWS
        chosen = jnp.max(jnp.where(place == own, 1.0, 0.0), axis=1, keepdims=True) > 0.0
        old_key = old[0, part, :].astype(f32)
        old_value = old[1, part, :].astype(f32)
        new_key = acc_kv[part, :HEAD_DIM]
        new_value = acc_kv[part, HEAD_DIM:]
        kv_out[part, :] = jnp.where(chosen, new_key, old_key).astype(bf16)
        kv_out[TOK + t * ROWS:TOK + (t + 1) * ROWS, :] = jnp.where(chosen, new_value, old_value).T.astype(bf16)
        shift = (new_key - old_key) ** 2 + (new_value - old_value) ** 2
        dev = jnp.sum(shift.T, axis=0, keepdims=True)
        dev_out[t:t + 1, :] = dev
        at = lane + (first + t * ROWS)
        doc = sum([(at >= e).astype(jnp.int32) for e in ends])
        for d in range(DOCS):
            totals[d] = totals[d] + jnp.where(doc == d, dev, 0.0)
    row = jnp.zeros((1, ROWS), f32)
    for d in range(DOCS):
        row = jnp.where(lane == d, jnp.sum(totals[d], axis=1, keepdims=True), row)
    dev_out[6:7, :] = row
    dev_out[7:8, :] = jnp.zeros((1, ROWS), f32)


def project(lengths, selected, hidden, w_query, w_key, w_value, cached_key, cached_value):
    steps = hidden.shape[1] // CHUNK
    hbm = pl.BlockSpec(memory_space=pltpu.HBM)
    vmem = pl.BlockSpec(memory_space=pltpu.VMEM)
    return pl.pallas_call(
        project_kernel,
        in_specs=[pl.BlockSpec(memory_space=pltpu.SMEM)] + [hbm] * 7,
        out_specs=[vmem] * 4,
        out_shape=[
            jax.ShapeDtypeStruct((KV_ROWS, HEAD_DIM), bf16),
            jax.ShapeDtypeStruct((QROWS, HEAD_DIM), bf16),
            jax.ShapeDtypeStruct((8, ROWS), f32),
            jax.ShapeDtypeStruct((1, QROWS), jnp.int32),
        ],
        scratch_shapes=[
            pltpu.VMEM((steps, TOK, CHUNK), bf16),
            pltpu.VMEM((steps, CHUNK, GROUP * HEAD_DIM), bf16),
            pltpu.VMEM((steps, CHUNK, 2 * HEAD_DIM), bf16),
            pltpu.VMEM((2, TOK, HEAD_DIM), bf16),
            pltpu.SMEM(selected.shape, jnp.int32),
            pltpu.VMEM((TOK, 2 * HEAD_DIM), f32),
            pltpu.VMEM((ROWS, GROUP * HEAD_DIM), f32),
            pltpu.SemaphoreType.DMA((4, steps)),
            pltpu.SemaphoreType.DMA((3,)),
        ],
        compiler_params=pltpu.CompilerParams(vmem_limit_bytes=VMEM_PROJECT),
        cost_estimate=pl.CostEstimate(flops=5 * 10**9, bytes_accessed=13 * 10**6, transcendentals=0),
        name="project",
    )(lengths, selected, hidden, w_query, w_key, w_value, cached_key, cached_value)


X_STEPS = (0, 1, 3, 2)
Y_STEPS = (0, 1, 3, 2)
ACC = HEAD_DIM + 16


def score_tile(q, kv, i, j, s_ref, top_ref):
    s = lax.dot_general(kv[j, :TOK, :], q[i], (((1,), (1,)), ((), ())), preferred_element_type=f32)
    s_ref[...] = s
    top_ref[...] = jnp.max(s.reshape(TOK // 8, 8, QROWS), axis=0)


def mix_tile(kv, m_s, acc_s, i, j, s_ref, top_ref):
    old = m_s[i, 0:1, :]
    new = jnp.maximum(old, jnp.max(top_ref[...], axis=0, keepdims=True))
    m_s[i, 0:1, :] = new
    p = jnp.exp2(s_ref[...] - new).astype(bf16)
    values = jnp.concatenate(
        [kv[j, TOK + k * ROWS:TOK + (k + 1) * ROWS, :] for k in range(TOK // ROWS)], axis=1)
    values = jnp.concatenate([values, jnp.ones((16, TOK), bf16)], axis=0)
    acc_s[i] = acc_s[i] * jnp.exp2(old - new) + jnp.dot(values, p, preferred_element_type=f32)


def add_kernel(a, b, out):
    out[...] = a[...] + b[...]


def small(kernel, *args):
    vmem = pl.BlockSpec(memory_space=pltpu.VMEM)
    return pl.pallas_call(
        kernel,
        in_specs=[vmem] * len(args),
        out_specs=vmem,
        out_shape=jax.ShapeDtypeStruct((8, ROWS), f32),
        compiler_params=pltpu.CompilerParams(vmem_limit_bytes=4 * 2**20),
        cost_estimate=pl.CostEstimate(flops=10**6, bytes_accessed=10**4, transcendentals=0),
    )(*args)


def attend_kernel(steps, first, last, *refs):
    n = 2 * len(steps)
    refs = list(refs)
    mask_rows = refs.pop(0) if first else None
    docs = refs.pop(0) if last else None
    q_in, refs = refs[:4], refs[4:]
    kv_in, refs = refs[:n], refs[n:]
    own_kv = refs.pop(0) if first else None
    if not first:
        m_in, acc_in, refs = refs[0], refs[1], refs[2:]
    if last:
        outs, refs = refs[:4], refs[4:]
        m_s, acc_s, refs = refs[0], refs[1], refs[2:]
    else:
        m_s, acc_s, refs = refs[0], refs[1], refs[2:]
    q, kv, s_a, s_b, top_a, top_b, pairs = refs
    for i in range(4):
        q[i] = q_in[i][...]
    x, y, c = lax.axis_index("x"), lax.axis_index("y"), lax.axis_index("c")
    for side in range(2):
        @pl.when(c == side)
        def _():
            for j in range(n):
                kv[j] = kv_in[j ^ side][...]

    if first:
        kv[n] = own_kv[...]
        m_s[...] = jnp.full_like(m_s, NEG)
        acc_s[...] = jnp.zeros_like(acc_s)
        place = lax.broadcasted_iota(jnp.int32, (TOK, QROWS), 0)
        s = lax.dot_general(kv[n, :TOK, :], q[0], (((1,), (1,)), ((), ())), preferred_element_type=f32)
        s = jnp.where(place <= mask_rows[...], s, NEG)
        s_a[...] = s
        top_a[...] = jnp.max(s.reshape(TOK // 8, 8, QROWS), axis=0)
        mix_tile(kv, m_s, acc_s, 0, n, s_a, top_a)
    else:
        m_s[...] = m_in[...]
        acc_s[...] = acc_in[...]
    count = jnp.int32(0)
    for i, dx in enumerate(X_STEPS):
        for j in range(n):
            q_at = ((x + dx) & 3) * 8 + 2 * y + c
            kv_at = (3 - x if j % 2 else x) * 8 + 2 * ((y + steps[j // 2]) & 3) + j % 2
            pairs[count] = i * 8 + j
            count = count + jnp.where(q_at > kv_at, 1, 0)

    def pair(k):
        v = pairs[jnp.minimum(k, count - 1)]
        return v >> 3, v & 7

    @pl.when(count > 0)
    def _():
        score_tile(q, kv, *pair(0), s_a, top_a)

    @pl.loop(0, (count + 1) >> 1)
    def _(h):
        k = h * 2
        score_tile(q, kv, *pair(k + 1), s_b, top_b)
        mix_tile(kv, m_s, acc_s, *pair(k), s_a, top_a)

        @pl.when(k + 1 < count)
        def _():
            score_tile(q, kv, *pair(k + 2), s_a, top_a)
            mix_tile(kv, m_s, acc_s, *pair(k + 1), s_b, top_b)

    if last:
        pieces = [jnp.concatenate([v] * GROUP, axis=1) for v in split3(docs[6:7, :])]
        for i in range(4):
            total = acc_s[i, HEAD_DIM:HEAD_DIM + 1, :]
            safe = jnp.maximum(total, 1e-30)
            outs[i][:HEAD_DIM, :] = (acc_s[i, :HEAD_DIM, :] * (1.0 / safe)).astype(bf16)
            lse = jnp.where(total > 0.0, m_s[i, 0:1, :] + jnp.log2(safe), NEG)
            outs[i][HEAD_DIM:, :] = jnp.concatenate(
                split3(lse) + pieces + [jnp.zeros((10, QROWS), f32)], axis=0).astype(bf16)


def split3(value):
    high = value.astype(bf16).astype(f32)
    mid = (value - high).astype(bf16).astype(f32)
    return [high, mid, value - high - mid]


def attend(steps, qs, kvs, mask_rows=None, own_kv=None, state=None, docs=None):
    first, last = state is None, docs is not None
    n = 2 * len(steps)
    vmem = pl.BlockSpec(memory_space=pltpu.VMEM)
    args = ([mask_rows] if first else []) + ([docs] if last else []) + list(qs) + list(kvs)
    args += [own_kv] if first else list(state)
    states = [jax.ShapeDtypeStruct((4, 8, QROWS), f32), jax.ShapeDtypeStruct((4, ACC, QROWS), f32)]
    keep = [pltpu.VMEM((4, 8, QROWS), f32), pltpu.VMEM((4, ACC, QROWS), f32)]
    return pl.pallas_call(
        functools.partial(attend_kernel, steps, first, last),
        in_specs=[vmem] * len(args),
        out_specs=[vmem] * (4 if last else 2),
        out_shape=[jax.ShapeDtypeStruct((ACC, QROWS), bf16)] * 4 if last else states,
        scratch_shapes=(keep if last else []) + [
            pltpu.VMEM((4, QROWS, HEAD_DIM), bf16),
            pltpu.VMEM((n + (1 if first else 0), KV_ROWS, HEAD_DIM), bf16),
            pltpu.VMEM((TOK, QROWS), f32),
            pltpu.VMEM((TOK, QROWS), f32),
            pltpu.VMEM((8, QROWS), f32),
            pltpu.VMEM((8, QROWS), f32),
            pltpu.SMEM((40,), jnp.int32),
        ],
        compiler_params=pltpu.CompilerParams(vmem_limit_bytes=30 * 2**20),
        cost_estimate=pl.CostEstimate(flops=n * 4 * 10**9, bytes_accessed=4 * 10**6, transcendentals=10**6),
        name="attend",
    )(*args)


def combine_kernel(lengths, dev, p0, p1, p2, p3, out, score):
    parts = (p0, p1, p2, p3)
    rows = [p[HEAD_DIM:HEAD_DIM + 16, :].astype(f32) for p in parts]
    lses = [v[0:1] + v[1:2] + v[2:3] for v in rows]
    total = sum([v[3:4, :ROWS] + v[4:5, :ROWS] + v[5:6, :ROWS] for v in rows])
    top = functools.reduce(jnp.maximum, lses)
    weights = [jnp.exp2(v - top) for v in lses]
    scale = 1.0 / sum(weights)
    mixed = sum([p[:HEAD_DIM, :].astype(f32) * (w * scale) for p, w in zip(parts, weights)])
    for h in range(GROUP):
        out[:, h * HEAD_DIM:(h + 1) * HEAD_DIM] = (
            mixed[:, h * ROWS:(h + 1) * ROWS].T[:SEL, :].astype(bf16))
    first = seq_number() * TOK
    ends = doc_ends(lengths)
    lane = lax.broadcasted_iota(jnp.int32, (8, ROWS), 1)
    place = lane + lax.broadcasted_iota(jnp.int32, (8, ROWS), 0) * ROWS + first
    doc = sum([(place >= e).astype(jnp.int32) for e in ends])
    mean = jnp.zeros((8, ROWS), f32)
    for d in range(DOCS):
        mean = jnp.where(doc == d, total[:, d:d + 1] / lengths[d].astype(f32), mean)
    score[...] = dev[...] / (mean + 1.0)


def combine(lengths, dev, parts):
    vmem = pl.BlockSpec(memory_space=pltpu.VMEM)
    return pl.pallas_call(
        combine_kernel,
        in_specs=[pl.BlockSpec(memory_space=pltpu.SMEM)] + [vmem] * 5,
        out_specs=[vmem, vmem],
        out_shape=[
            jax.ShapeDtypeStruct((SEL, GROUP * HEAD_DIM), bf16),
            jax.ShapeDtypeStruct((8, ROWS), f32),
        ],
        compiler_params=pltpu.CompilerParams(vmem_limit_bytes=8 * 2**20),
        cost_estimate=pl.CostEstimate(flops=10**6, bytes_accessed=10**6, transcendentals=0),
        name="combine",
    )(lengths, dev, *parts)


def fetch(value, axis, step):
    size = lax.axis_size(axis)
    return lax.ppermute(value, axis, [((i + step) % size, i) for i in range(size)])


def between(value, target):
    moves = []
    for x in range(4):
        for y in range(4):
            for c in range(2):
                to = target(x, y, c)
                if to is not None:
                    moves.append(((x * 4 + y) * 2 + c, (to[0] * 4 + to[1]) * 2 + to[2]))
    return lax.ppermute(value, SEQ, moves)


def exchange(value, axis, bit):
    size = lax.axis_size(axis)
    return lax.ppermute(value, axis, [(i, i ^ bit) for i in range(size)])


def program(hidden, w_query, w_key, w_value, cached_key, cached_value, doc_lengths, selected):
    kv, q, dev, mask_rows = project(
        doc_lengths, selected, hidden, w_query, w_key, w_value, cached_key, cached_value)
    kept, other, qs = {}, {}, [q]
    for s in Y_STEPS:
        kept[s] = between(kv, lambda x, y, c: (3 - x if c else x, (y - s) % 4, c))
    for s in Y_STEPS:
        other[s] = exchange(kept[s], "c", 1)
    for s in X_STEPS[1:]:
        qs.append(fetch(q, "x", s))
    for bit in (1, 2, 4):
        dev = small(add_kernel, dev, exchange(dev, "kvh", bit))
    for axis, bit in (("c", 1), ("y", 1), ("y", 2)):
        docs = dev if axis == "c" else docs
        docs = small(add_kernel, docs, exchange(docs, axis, bit))
    state = None
    for n, steps in enumerate(KERNELS):
        first, last = n == 0, n == len(KERNELS) - 1
        kvs = sum([[kept[s], other[s]] for s in steps], [])
        state = attend(steps, qs, kvs, mask_rows if first else None, kv if first else None, state,
                       docs if last else None)
    mine = [state[0]]
    for n, s in enumerate(X_STEPS[1:]):
        mine.append(fetch(state[n + 1], "x", (4 - s) % 4))
    attended, score = combine(doc_lengths, dev, mine)
    return attended, score.reshape(-1)[:TOK]


KERNELS = ((0,), (1,), (3,), (2,))


def solution(mesh):
    fine = Mesh(mesh.devices.reshape(4, 4, 2, 8), ("x", "y", "c", "kvh"))
    return jax.shard_map(
        program,
        mesh=fine,
        in_specs=(
            P(SEQ, None),
            P(None, "kvh"),
            P(None, "kvh"),
            P(None, "kvh"),
            P(SEQ, "kvh"),
            P(SEQ, "kvh"),
            P(),
            P(),
        ),
        out_specs=(P(SEQ, "kvh"), P(SEQ)),
        check_vma=False,
    )
```

```python
import functools
import math

import jax
import jax.numpy as jnp
from jax import lax
from jax.experimental import pallas as pl
from jax.experimental.pallas import tpu as pltpu
from jax.sharding import Mesh, PartitionSpec as P


KV_HEADS = 8
HEAD_DIM = 128
GROUP = 4
TOK = 768
SEL = 120
ROWS = 128
QROWS = GROUP * ROWS
DOCS = 4
CHUNK = 512
NEG = -1e30
VMEM_PROJECT = 24 * 2**20
KV_ROWS = 2 * TOK
EXP_SCALE = (HEAD_DIM ** -0.5) * math.log2(math.e)
SEQ = ("x", "y", "c")
f32, bf16 = jnp.float32, jnp.bfloat16


def seq_number():
    return (lax.axis_index("x") * 4 + lax.axis_index("y")) * 2 + lax.axis_index("c")


def doc_ends(lengths):
    ends = [lengths[0]]
    for d in range(1, DOCS):
        ends.append(ends[-1] + lengths[d])
    return ends


def project_kernel(lengths_in, selected, hidden, w_query, w_key, w_value, cached_key, cached_value,
                   kv_out, q_out, dev_out, mask_out,
                   states, wq, wkv, old, lengths, chosen_rows, picked, acc_kv, acc_q, sem, one_sem):
    steps = hidden.shape[1] // CHUNK
    fetch_rows = pltpu.make_async_copy(selected, chosen_rows, one_sem.at[0])
    fetch_rows.start()
    fetch_lengths = pltpu.make_async_copy(lengths_in, lengths, one_sem.at[3])
    fetch_lengths.start()
    copies = []
    for k in range(steps):
        part = pl.ds(k * CHUNK, CHUNK)
        copies.append([
            pltpu.make_async_copy(hidden.at[:, part], states.at[k], sem.at[0, k]),
            pltpu.make_async_copy(w_key.at[part, :], wkv.at[k, :, pl.ds(0, HEAD_DIM)], sem.at[1, k]),
            pltpu.make_async_copy(w_value.at[part, :], wkv.at[k, :, pl.ds(HEAD_DIM, HEAD_DIM)], sem.at[2, k]),
        ])
        for copy in copies[-1]:
            copy.start()
    olds = [
        pltpu.make_async_copy(cached_key, old.at[0], one_sem.at[1]),
        pltpu.make_async_copy(cached_value, old.at[1], one_sem.at[2]),
    ]
    for copy in olds:
        copy.start()
    late = [pltpu.make_async_copy(w_query.at[pl.ds(k * CHUNK, CHUNK), :], wq.at[k], sem.at[3, k]) for k in range(steps)]
    for copy in late:
        copy.start()

    def fresh(k):
        for copy in copies[k]:
            copy.wait()
        product = jnp.dot(states[k], wkv[k], preferred_element_type=f32)
        acc_kv[...] = product if k == 0 else acc_kv[...] + product

    half = steps // 2
    for k in range(half):
        fresh(k)
    fetch_rows.wait()
    base = seq_number() * SEL
    lane = lax.broadcasted_iota(jnp.int32, (1, ROWS), 1)
    pieces = [jnp.full((1, ROWS), -1, jnp.int32) for _ in range(4)]
    for r in range(SEL):
        pieces[r % 4] = jnp.where(lane == r, chosen_rows[base + r], pieces[r % 4])
    own = functools.reduce(jnp.maximum, pieces)
    mask_out[...] = jnp.concatenate([jnp.where(lane < SEL, own, TOK)] * GROUP, axis=1)
    across = jnp.broadcast_to(own, (ROWS, ROWS)).astype(f32).T
    tokens = lax.broadcasted_iota(jnp.int32, (ROWS, TOK), 1).astype(f32)
    pick = jnp.where(jnp.concatenate([across] * (TOK // ROWS), axis=1) == tokens, 1.0, 0.0).astype(bf16)
    for k in range(half, steps):
        fresh(k)
        for j in (k - half, k):
            picked[j] = jnp.dot(pick, states[j], preferred_element_type=f32).astype(bf16)
    for copy in olds:
        copy.wait()
    fetch_lengths.wait()
    first = seq_number() * TOK
    ends = doc_ends(lengths)
    totals = [jnp.zeros((1, ROWS), f32) for _ in range(DOCS)]
    for t in range(TOK // ROWS):
        part = slice(t * ROWS, (t + 1) * ROWS)
        place = lax.broadcasted_iota(jnp.int32, (ROWS, ROWS), 0) + t * ROWS
        chosen = jnp.max(jnp.where(place == own, 1.0, 0.0), axis=1, keepdims=True) > 0.0
        old_key = old[0, part, :].astype(f32)
        old_value = old[1, part, :].astype(f32)
        new_key = acc_kv[part, :HEAD_DIM]
        new_value = acc_kv[part, HEAD_DIM:]
        kv_out[part, :] = jnp.where(chosen, new_key, old_key).astype(bf16)
        kv_out[TOK + t * ROWS:TOK + (t + 1) * ROWS, :] = jnp.where(chosen, new_value, old_value).T.astype(bf16)
        shift = (new_key - old_key) ** 2 + (new_value - old_value) ** 2
        dev = jnp.sum(shift.T, axis=0, keepdims=True)
        for z in range(KV_HEADS):
            dev_out[z, t:t + 1, :] = dev
        at = lane + (first + t * ROWS)
        doc = sum([(at >= e).astype(jnp.int32) for e in ends])
        for d in range(DOCS):
            totals[d] = totals[d] + jnp.where(doc == d, dev, 0.0)
    row = jnp.zeros((1, ROWS), f32)
    for d in range(DOCS):
        row = jnp.where(lane == d, jnp.sum(totals[d], axis=1, keepdims=True), row)
    for z in range(KV_HEADS):
        dev_out[z, 6:7, :] = row
        dev_out[z, 7:8, :] = jnp.zeros((1, ROWS), f32)
    for k in range(steps):
        late[k].wait()
        product = jnp.dot(picked[k], wq[k], preferred_element_type=f32)
        acc_q[...] = product if k == 0 else acc_q[...] + product
    for h in range(GROUP):
        q_out[h * ROWS:(h + 1) * ROWS, :] = (
            acc_q[:, h * HEAD_DIM:(h + 1) * HEAD_DIM] * EXP_SCALE).astype(bf16)


def project(lengths, selected, hidden, w_query, w_key, w_value, cached_key, cached_value):
    steps = hidden.shape[1] // CHUNK
    hbm = pl.BlockSpec(memory_space=pltpu.HBM)
    vmem = pl.BlockSpec(memory_space=pltpu.VMEM)
    return pl.pallas_call(
        project_kernel,
        in_specs=[hbm] * 8,
        out_specs=[vmem] * 4,
        out_shape=[
            jax.ShapeDtypeStruct((KV_ROWS, HEAD_DIM), bf16),
            jax.ShapeDtypeStruct((QROWS, HEAD_DIM), bf16),
            jax.ShapeDtypeStruct((KV_HEADS, 8, ROWS), f32),
            jax.ShapeDtypeStruct((1, QROWS), jnp.int32),
        ],
        scratch_shapes=[
            pltpu.VMEM((steps, TOK, CHUNK), bf16),
            pltpu.VMEM((steps, CHUNK, GROUP * HEAD_DIM), bf16),
            pltpu.VMEM((steps, CHUNK, 2 * HEAD_DIM), bf16),
            pltpu.VMEM((2, TOK, HEAD_DIM), bf16),
            pltpu.SMEM(lengths.shape, jnp.int32),
            pltpu.SMEM(selected.shape, jnp.int32),
            pltpu.VMEM((steps, ROWS, CHUNK), bf16),
            pltpu.VMEM((TOK, 2 * HEAD_DIM), f32),
            pltpu.VMEM((ROWS, GROUP * HEAD_DIM), f32),
            pltpu.SemaphoreType.DMA((4, steps)),
            pltpu.SemaphoreType.DMA((4,)),
        ],
        compiler_params=pltpu.CompilerParams(vmem_limit_bytes=VMEM_PROJECT),
        cost_estimate=pl.CostEstimate(flops=5 * 10**9, bytes_accessed=13 * 10**6, transcendentals=0),
        name="project",
    )(*[pltpu.with_memory_space_constraint(v, pltpu.HBM) for v in (
        lengths, selected, hidden, w_query, w_key, w_value, cached_key, cached_value)])


X_STEPS = (0, 1, 3, 2)
Y_STEPS = (0, 1, 3, 2)
ACC = HEAD_DIM + 16


def score_tile(q, kv, i, j, s_ref, top_ref):
    s = lax.dot_general(kv[j, :TOK, :], q[i], (((1,), (1,)), ((), ())), preferred_element_type=f32)
    s_ref[...] = s
    top_ref[...] = jnp.max(s.reshape(TOK // 8, 8, QROWS), axis=0)


def mix_tile(kv, m_s, acc_s, i, j, s_ref, top_ref):
    old = m_s[i, 0:1, :]
    new = jnp.maximum(old, jnp.max(top_ref[...], axis=0, keepdims=True))
    m_s[i, 0:1, :] = new
    p = jnp.exp2(s_ref[...] - new).astype(bf16)
    values = jnp.concatenate(
        [kv[j, TOK + k * ROWS:TOK + (k + 1) * ROWS, :] for k in range(TOK // ROWS)], axis=1)
    values = jnp.concatenate([values, jnp.ones((16, TOK), bf16)], axis=0)
    acc_s[i] = acc_s[i] * jnp.exp2(old - new) + jnp.dot(values, p, preferred_element_type=f32)


def sum_kernel(a, out):
    out[...] = sum([a[z] for z in range(KV_HEADS)])


def add_kernel(a, b, out):
    out[...] = a[...] + b[...]


def small(kernel, *args):
    vmem = pl.BlockSpec(memory_space=pltpu.VMEM)
    return pl.pallas_call(
        kernel,
        in_specs=[vmem] * len(args),
        out_specs=vmem,
        out_shape=jax.ShapeDtypeStruct((8, ROWS), f32),
        compiler_params=pltpu.CompilerParams(vmem_limit_bytes=4 * 2**20),
        cost_estimate=pl.CostEstimate(flops=10**6, bytes_accessed=10**4, transcendentals=0),
    )(*args)


def attend_kernel(steps, mine, first, last, *refs):
    n, r = 2 * len(steps), len(mine)
    refs = list(refs)

    def take(count):
        return [refs.pop(0) for _ in range(count)]

    q_in, kv_in = take(r), take(n)
    if first:
        mask_rows, = take(1)
    else:
        m_in, acc_in = take(r), take(r)
    if last:
        docs, = take(1)
        outs = take(r)
        pieces = [jnp.concatenate([v] * GROUP, axis=1) for v in split3(docs[6:7, :])]
    else:
        m_out, acc_out = take(r), take(r)
    q, kv, m_s, acc_s, s_a, s_b, top_a, top_b, pairs = refs
    for i in range(r):
        q[i] = q_in[i][...]
    x, y, c = lax.axis_index("x"), lax.axis_index("y"), lax.axis_index("c")
    for side in range(2):
        @pl.when(c == side)
        def _():
            for j in range(n):
                kv[j] = kv_in[j ^ side][...]

    if first:
        m_s[...] = jnp.full_like(m_s, NEG)
        acc_s[...] = jnp.zeros_like(acc_s)
        place = lax.broadcasted_iota(jnp.int32, (TOK, QROWS), 0)
        s = lax.dot_general(kv[c, :TOK, :], q[0], (((1,), (1,)), ((), ())), preferred_element_type=f32)
        s = jnp.where(place <= mask_rows[...], s, NEG)
        s_a[...] = s
        top_a[...] = jnp.max(s.reshape(TOK // 8, 8, QROWS), axis=0)
        mix_tile(kv, m_s, acc_s, 0, c, s_a, top_a)
    else:
        for i in range(r):
            m_s[i] = m_in[i][...]
            acc_s[i] = acc_in[i][...]
    count = jnp.int32(0)
    for i in range(r):
        for j in range(n):
            step = steps[j // 2]
            q_at = ((x + X_STEPS[mine[i]]) & 3) * 8 + 2 * y + c
            kv_at = (3 - x if step and j % 2 else x) * 8 + 2 * ((y + step) & 3) + j % 2
            pairs[count] = i * 8 + j
            count = count + jnp.where(q_at > kv_at, 1, 0)

    def pair(k):
        v = pairs[jnp.minimum(k, count - 1)]
        return v >> 3, v & 7

    @pl.when(count > 0)
    def _():
        score_tile(q, kv, *pair(0), s_a, top_a)

    @pl.loop(0, (count + 1) >> 1)
    def _(h):
        k = h * 2
        score_tile(q, kv, *pair(k + 1), s_b, top_b)
        mix_tile(kv, m_s, acc_s, *pair(k), s_a, top_a)

        @pl.when(k + 1 < count)
        def _():
            score_tile(q, kv, *pair(k + 2), s_a, top_a)
            mix_tile(kv, m_s, acc_s, *pair(k + 1), s_b, top_b)

    for i in range(r):
        if last:
            total = acc_s[i, HEAD_DIM:HEAD_DIM + 1, :]
            safe = jnp.maximum(total, 1e-30)
            outs[i][:HEAD_DIM, :] = (acc_s[i, :HEAD_DIM, :] * (1.0 / safe)).astype(bf16)
            lse = jnp.where(total > 0.0, m_s[i, 0:1, :] + jnp.log2(safe), NEG)
            outs[i][HEAD_DIM:, :] = jnp.concatenate(
                split3(lse) + pieces + [jnp.zeros((10, QROWS), f32)], axis=0).astype(bf16)
        else:
            m_out[i][...] = m_s[i]
            acc_out[i][...] = acc_s[i]


def split3(value):
    high = value.astype(bf16).astype(f32)
    mid = (value - high).astype(bf16).astype(f32)
    return [high, mid, value - high - mid]


def attend(steps, mine, last, qs, kvs, extra):
    first = extra[0].dtype == jnp.int32
    n, r = 2 * len(steps), len(mine)
    vmem = pl.BlockSpec(memory_space=pltpu.VMEM)
    args = list(qs) + list(kvs) + list(extra)
    if last:
        results = [jax.ShapeDtypeStruct((ACC, QROWS), bf16)] * r
    else:
        results = [jax.ShapeDtypeStruct((8, QROWS), f32)] * r + [jax.ShapeDtypeStruct((ACC, QROWS), f32)] * r
    return pl.pallas_call(
        functools.partial(attend_kernel, steps, mine, first, last),
        in_specs=[vmem] * len(args),
        out_specs=[vmem] * len(results),
        out_shape=results,
        scratch_shapes=[
            pltpu.VMEM((r, QROWS, HEAD_DIM), bf16),
            pltpu.VMEM((n, KV_ROWS, HEAD_DIM), bf16),
            pltpu.VMEM((r, 8, QROWS), f32),
            pltpu.VMEM((r, ACC, QROWS), f32),
            pltpu.VMEM((TOK, QROWS), f32),
            pltpu.VMEM((TOK, QROWS), f32),
            pltpu.VMEM((8, QROWS), f32),
            pltpu.VMEM((8, QROWS), f32),
            pltpu.SMEM((40,), jnp.int32),
        ],
        compiler_params=pltpu.CompilerParams(vmem_limit_bytes=14 * 2**20),
        cost_estimate=pl.CostEstimate(flops=n * r * 10**9, bytes_accessed=4 * 10**6, transcendentals=10**6),
        name="attend",
    )(*args)


def combine_kernel(lengths, dev, p0, p1, p2, p3, out, score):
    parts = (p0, p1, p2, p3)
    rows = [p[HEAD_DIM:HEAD_DIM + 16, :].astype(f32) for p in parts]
    lses = [v[0:1] + v[1:2] + v[2:3] for v in rows]
    total = sum([v[3:4, :ROWS] + v[4:5, :ROWS] + v[5:6, :ROWS] for v in rows])
    top = functools.reduce(jnp.maximum, lses)
    weights = [jnp.exp2(v - top) for v in lses]
    scale = 1.0 / sum(weights)
    mixed = sum([p[:HEAD_DIM, :].astype(f32) * (w * scale) for p, w in zip(parts, weights)])
    for h in range(GROUP):
        out[:, h * HEAD_DIM:(h + 1) * HEAD_DIM] = (
            mixed[:, h * ROWS:(h + 1) * ROWS].T[:SEL, :].astype(bf16))
    first = seq_number() * TOK
    ends = doc_ends(lengths)
    lane = lax.broadcasted_iota(jnp.int32, (8, ROWS), 1)
    place = lane + lax.broadcasted_iota(jnp.int32, (8, ROWS), 0) * ROWS + first
    doc = sum([(place >= e).astype(jnp.int32) for e in ends])
    mean = jnp.zeros((8, ROWS), f32)
    for d in range(DOCS):
        mean = jnp.where(doc == d, total[:, d:d + 1] / lengths[d].astype(f32), mean)
    value = dev[...] / (mean + 1.0)
    for t in range(TOK // ROWS):
        score[pl.ds(t * ROWS, ROWS)] = value[t]


def combine(lengths, dev, parts):
    vmem = pl.BlockSpec(memory_space=pltpu.VMEM)
    return pl.pallas_call(
        combine_kernel,
        in_specs=[pl.BlockSpec(memory_space=pltpu.SMEM)] + [vmem] * 5,
        out_specs=[vmem, vmem],
        out_shape=[
            jax.ShapeDtypeStruct((SEL, GROUP * HEAD_DIM), bf16),
            jax.ShapeDtypeStruct((TOK,), f32),
        ],
        compiler_params=pltpu.CompilerParams(vmem_limit_bytes=8 * 2**20),
        cost_estimate=pl.CostEstimate(flops=10**6, bytes_accessed=10**6, transcendentals=0),
        name="combine",
    )(lengths, dev, *parts)


def fetch(value, axis, step):
    size = lax.axis_size(axis)
    return lax.ppermute(value, axis, [((i + step) % size, i) for i in range(size)])


def between(value, target):
    moves = []
    for x in range(4):
        for y in range(4):
            for c in range(2):
                to = target(x, y, c)
                if to is not None:
                    moves.append(((x * 4 + y) * 2 + c, (to[0] * 4 + to[1]) * 2 + to[2]))
    return lax.ppermute(value, SEQ, moves)


def exchange(value, axis, bit):
    size = lax.axis_size(axis)
    return lax.ppermute(value, axis, [(i, i ^ bit) for i in range(size)])


def program(hidden, w_query, w_key, w_value, cached_key, cached_value, doc_lengths, selected):
    kv, q, dev, mask_rows = project(
        doc_lengths, selected, hidden, w_query, w_key, w_value, cached_key, cached_value)
    kept, other, qs = {0: kv}, {}, [q]
    for s in Y_STEPS[1:]:
        kept[s] = between(kv, lambda x, y, c: (3 - x if c else x, (y - s) % 4, c))
    for s in Y_STEPS:
        other[s] = exchange(kept[s], "c", 1)
    for s in X_STEPS[1:]:
        qs.append(fetch(q, "x", s))
    dev = small(sum_kernel, lax.all_to_all(dev, "kvh", 0, 0, tiled=True))
    docs = small(add_kernel, dev, exchange(dev, "c", 1))
    for bit in (1, 2):
        docs = small(add_kernel, docs, exchange(docs, "y", bit))
    state = [mask_rows]
    for steps in KERNELS[:-1]:
        kvs = sum([[kept[s], other[s]] for s in steps], [])
        state = attend(steps, (0, 1, 2, 3), False, qs, kvs, state)
    kvs = sum([[kept[s], other[s]] for s in KERNELS[-1]], [])
    mine = {}
    for n in (3, 1, 2, 0):
        s = X_STEPS[n]
        part, = attend(KERNELS[-1], (n,), True, [qs[n]], kvs, [state[n], state[4 + n], docs])
        mine[s] = fetch(part, "x", (4 - s) % 4) if s else part
    mine = [mine[s] for s in X_STEPS]
    attended, score = combine(doc_lengths, dev, mine)
    return attended, score


KERNELS = ((0,), (1,), (3,), (2,))


def solution(mesh):
    fine = Mesh(mesh.devices.reshape(4, 4, 2, 8), ("x", "y", "c", "kvh"))
    return jax.shard_map(
        program,
        mesh=fine,
        in_specs=(
            P(SEQ, None),
            P(None, "kvh"),
            P(None, "kvh"),
            P(None, "kvh"),
            P(SEQ, "kvh"),
            P(SEQ, "kvh"),
            P(),
            P(),
        ),
        out_specs=(P(SEQ, "kvh"), P(SEQ)),
        check_vma=False,
    )
```
